128 devices in a mesh: row: 8 (over x, z_lo), col: 16 (over z_hi, y, core).
Axes of the slice: x: 4, y: 4, z: 4 (z_hi: 2, z_lo: 2; z = z_hi * 2 + z_lo), core: 2. Of those that a mesh axis runs over, the one named last changes fastest.
Arguments:
- dosages: bfloat16 [4, 1024, 65536], P(None, ('row', 'col')), may hold values from 0 to 2
- allele_counts: int32 [4, 1024], replicated, may hold values from 58982 to 72088
- slab_in: float32 [4096, 65536], P('row', 'col'), may hold values from -6 to 6
Outputs:
- slab_out: float32 [4096, 65536], P('row', 'col')
The draws below stay inside these ranges and needn't reach their ends.
All inputs are finite; a program needn't handle non-finite values.
Results may differ from the reference program's by a relative error of at most 0.002.
Values may be sent and summed in bfloat16 or wider, within the bound.
No kernel may reach another device: no remote copies, remote signals or barrier semaphores. Data moves between devices by JAX's collectives and lax.ppermute only.
A program may use at most 192 MiB of HBM per device.

```python
import math
import jax
import jax.numpy as jnp
from jax import lax

SNPS = 1024
GROUPS = 4
ROWS = 4096
SAMPLES = 65536


def set_ends(values, own_key, low, high):
    extent = values.shape
    spot = [jax.random.randint(jax.random.fold_in(own_key, axis), (), 0, extent[axis]) for axis in range(len(extent))]
    values = values.at[tuple(spot)].set(low)
    longest = extent.index(max(extent))
    spot[longest] = (spot[longest] + 1) % extent[longest]
    return values.at[tuple(spot)].set(high)


def shard_levels(own_key, extent, cuts, least, top_value):
    def one(axis_at, shards_of):
        heights = jax.random.uniform(jax.random.fold_in(jax.random.fold_in(own_key, 6), axis_at), (shards_of,), jnp.float32, least / len(cuts), top_value / len(cuts))
        return jnp.repeat(jnp.exp(heights), extent[axis_at] // shards_of).reshape((-1,) + (1,) * (len(extent) - axis_at - 1))

    level = one(*cuts[0])
    for cut in cuts[1:]:
        level = level * one(*cut)
    return level


def bell_draw(rng, shape, scale, bound, cuts=(), kind=jnp.bfloat16):
    entries = jax.random.normal(rng, shape, jnp.float32) * scale
    if len(cuts) > 0:
        entries = shard_levels(rng, shape, cuts, -0.22, 0.18) * entries
    return jnp.clip(entries, min=-bound, max=bound).astype(kind)


def setup_inputs(seed: int = 0) -> dict:
    key_list = jax.random.split(jax.random.key(seed), 4)
    return {
        "dosages": jnp.clip(2.0 * jax.random.uniform(key_list[0], (GROUPS, SNPS, SAMPLES), jnp.float32) ** shard_levels(key_list[0], (GROUPS, SNPS, SAMPLES), ((1, 128),), -0.2, 0.2), 0.0, 2.0).astype(jnp.bfloat16),
        "allele_counts": set_ends(jax.random.randint(key_list[1], (GROUPS, SNPS), 9 * SAMPLES // 10, 11 * SAMPLES // 10), jax.random.fold_in(key_list[1], 1), 9 * SAMPLES // 10, (11 * SAMPLES // 10) - 1).astype(jnp.int32),
        "slab_in": bell_draw(key_list[2], (ROWS, SAMPLES), 1.0, 6.0, ((0, 8), (1, 16)), jnp.float32),
    }


def standardize(dosage_block, count_row):
    frequency = count_row.astype(jnp.float32) / (2.0 * SAMPLES)
    centre = 2.0 * frequency
    spread = jnp.sqrt(2.0 * frequency * (1.0 - frequency))
    return ((dosage_block.astype(jnp.float32) - centre[:, None]) / spread[:, None]).astype(jnp.bfloat16)

def reference(dosages, allele_counts, slab_in):
    factor = 1.0 / math.sqrt(GROUPS * SNPS)
    total = slab_in
    for group_index in range(GROUPS):
        scaled = standardize(dosages[group_index], allele_counts[group_index]).astype(jnp.float32)
        product = jnp.dot(scaled[:, :ROWS].T, scaled, precision=lax.Precision.HIGHEST)
        total = total + factor * product
    return total
```

```python
import functools
import math

import jax
import jax.numpy as jnp
from jax import lax
from jax.experimental import pallas as pl
from jax.experimental.pallas import tpu as pltpu
from jax.sharding import Mesh, PartitionSpec as P

DEVICES = ("x", "zl", "zh", "y", "core")
RINGS = {"x": ("x", (0, 1, 2, 3)), "z": (("zl", "zh"), (0, 2, 1, 3)), "y": ("y", (0, 1, 2, 3))}
ORDERS = (("x", "y", "z"), ("y", "z", "x"), ("z", "x", "y"))
CHUNKS = 2
SENT = jnp.bfloat16


def neighbour(ring, by):
    axes, order = ring
    here = lax.axis_index(axes)
    found = [order[(order.index(i) + by) % len(order)] for i in range(len(order))]
    return sum(jnp.where(here == i, found[i], 0) for i in range(len(order)))


def ring_steps(block, ring):
    axes, order = ring
    axes = axes if isinstance(axes, tuple) else (axes,)
    pairs = []
    for i in range(len(order)):
        pairs.append((2 * order[i], 2 * order[(i + 1) % len(order)]))
        pairs.append((2 * order[i] + 1, 2 * order[i - 1] + 1))
    core = lax.axis_index("core")
    steps = []
    for step in range(1, len(order)):
        block = lax.ppermute(block, axes + ("core",), pairs)
        index = jnp.where(core == 0, neighbour(ring, -step), neighbour(ring, step))
        steps.append((block, index))
    return steps


def place(buffer, value, axis, index, lane=0):
    starts = [0] * buffer.ndim
    starts[axis], starts[-1] = index, lane
    return lax.dynamic_update_slice(buffer, jnp.expand_dims(value, axis), starts)


def gather_ring(block, ring, axis):
    buffer = jnp.broadcast_to(
        jnp.expand_dims(block, axis), block.shape[:axis] + (4,) + block.shape[axis:]
    )
    for value, index in ring_steps(block, ring):
        buffer = place(buffer, value, axis, index)
    return buffer


def gather_plane(block, order):
    for name, axis in ((order[0], 0), (order[1], int("xzy".index(order[0]) < "xzy".index(order[1])))):
        block = gather_ring(block, RINGS[name], axis)
    return block


def gather_last(blocks, orders):
    lanes = [0]
    for block in blocks:
        lanes.append(lanes[-1] + block.shape[-1])
    buffer = jnp.zeros((4, 4, 4, blocks[0].shape[2], lanes[-1]), blocks[0].dtype)
    rings = [RINGS[order[2]] for order in orders]
    held = [
        [(block, neighbour(ring, 0))] + ring_steps(block, ring)
        for block, ring in zip(blocks, rings, strict=True)
    ]
    for step in range(4):
        for i, order in enumerate(orders):
            value, index = held[i][step]
            buffer = place(buffer, value, "xzy".index(order[2]), index, lanes[i])
    return buffer


def spread_kernel(dosages, centre, inverse, *outs):
    groups, own, wide = dosages.shape
    values = dosages[...].astype(jnp.float32).reshape(groups * own, wide)
    values = ((values - centre[...]) * inverse[...]).astype(jnp.bfloat16)
    pieces, width = outs[0].shape[0], outs[0].shape[3]
    for k in range(pieces):
        for q, out in enumerate(outs):
            at = (k * len(outs) + q) * width
            out[k, 0] = values[:, at : at + width]


def spread_columns(dosages, centre, inverse, pieces, places, width):
    groups, own, _ = dosages.shape
    part = width // CHUNKS
    return pl.pallas_call(
        spread_kernel,
        grid=(places,),
        in_specs=[
            pl.BlockSpec((groups, own, pieces * width), lambda g: (0, 0, g)),
            pl.BlockSpec((groups * own, 1), lambda g: (0, 0)),
            pl.BlockSpec((groups * own, 1), lambda g: (0, 0)),
        ],
        out_specs=[pl.BlockSpec((pieces, 1, groups * own, part), lambda g: (0, g, 0, 0))] * CHUNKS,
        out_shape=[jax.ShapeDtypeStruct((pieces, places, groups * own, part), jnp.bfloat16)]
        * CHUNKS,
        cost_estimate=pl.CostEstimate(
            flops=4 * dosages.size, bytes_accessed=4 * dosages.size, transcendentals=0
        ),
        name="spread_columns",
    )(dosages, centre.reshape(-1, 1), inverse.reshape(-1, 1))


def multiply_kernel(scale, core, left, own, other, out):
    me = core[0]
    for slot, right in ((me, own), (1 - me, other)):
        product = lax.dot_general(
            left[...], right[...], (((0,), (0,)), ((), ())), preferred_element_type=jnp.float32
        )
        out[0, slot] = (scale * product).astype(out.dtype)


def multiply(left, own, other, core, blocks, scale):
    depth, width = own.shape
    rows = left.shape[1]
    height = rows // blocks
    return pl.pallas_call(
        functools.partial(multiply_kernel, scale),
        grid_spec=pltpu.PrefetchScalarGridSpec(
            num_scalar_prefetch=1,
            grid=(blocks,),
            in_specs=[
                pl.BlockSpec((depth, height), lambda b, c: (0, b)),
                pl.BlockSpec((depth, width), lambda b, c: (0, 0)),
                pl.BlockSpec((depth, width), lambda b, c: (0, 0)),
            ],
            out_specs=pl.BlockSpec((1, 2, height, width), lambda b, c: (b, 0, 0, 0)),
        ),
        out_shape=jax.ShapeDtypeStruct((blocks, 2, height, width), SENT),
        compiler_params=pltpu.CompilerParams(vmem_limit_bytes=48 * 2**20),
        cost_estimate=pl.CostEstimate(
            flops=4 * depth * rows * width,
            bytes_accessed=2 * depth * (rows + 2 * width) + 4 * rows * width,
            transcendentals=0,
        ),
        name="multiply",
    )(core, left, own, other)


def add_kernel(slab, *refs):
    *news, out = refs
    width = news[0].shape[3]
    for q, new in enumerate(news):
        _, cores, height, _ = new.shape
        for c in range(cores):
            at = (pl.ds(c * height, height), pl.ds(q * width, width))
            out[at] = slab[at] + new[0, c].astype(jnp.float32)


def add(slab, news):
    pieces, cores, height, width = news[0].shape
    wide = width * len(news)
    return pl.pallas_call(
        add_kernel,
        grid=(pieces,),
        in_specs=[pl.BlockSpec((cores * height, wide), lambda j: (0, j))]
        + [pl.BlockSpec((1, cores, height, width), lambda j: (j, 0, 0, 0))] * len(news),
        out_specs=pl.BlockSpec((cores * height, wide), lambda j: (0, j)),
        out_shape=jax.ShapeDtypeStruct(slab.shape, slab.dtype),
        cost_estimate=pl.CostEstimate(
            flops=2 * slab.size, bytes_accessed=10 * slab.size, transcendentals=0
        ),
        name="add_slab",
    )(slab, *news)


def local(dosages, allele_counts, slab_in):
    groups, own, samples = dosages.shape
    snps = allele_counts.shape[1]
    rows_n = lax.axis_size("x") * lax.axis_size("zl")
    cores = lax.axis_size("core")
    cols_n = lax.axis_size("zh") * lax.axis_size("y") * cores
    devices = rows_n * cols_n
    block_rows = slab_in.shape[0]
    rows = rows_n * block_rows
    width = samples // devices
    factor = 1.0 / math.sqrt(groups * snps)

    device = lax.axis_index(DEVICES)
    core = lax.axis_index("core")
    counts = lax.dynamic_slice(allele_counts, (0, device * own), (groups, own))
    frequency = counts.astype(jnp.float32) / (2.0 * samples)
    centre = 2.0 * frequency
    inverse = 1.0 / jnp.sqrt(2.0 * frequency * (1.0 - frequency))

    head = dosages[:, :, :rows].astype(jnp.float32)
    head = ((head - centre[:, :, None]) * inverse[:, :, None]).astype(jnp.bfloat16)
    head = head.reshape(groups * own, rows_n, cores, block_rows // cores)
    head = head.transpose(2, 0, 1, 3).reshape(cores, groups * own, rows // cores)
    head = lax.all_to_all(head, "core", split_axis=0, concat_axis=0, tiled=True)
    head = head.reshape(cores * groups * own, rows // cores)
    lanes = rows // cores // 128
    edges = [128 * -(-lanes * i // 3) for i in range(4)]
    planes = [
        gather_plane(head[:, edges[i] : edges[i + 1]], order) for i, order in enumerate(ORDERS)
    ]

    columns = spread_columns(dosages, centre, inverse, rows_n, cols_n, width)
    planes, columns = lax.optimization_barrier((planes, columns))
    left = gather_last(planes, ORDERS).reshape(groups * snps, rows // cores)
    news = []
    for part in columns:
        part = part.reshape(devices, groups * own, width // CHUNKS)
        mine = lax.all_to_all(part, DEVICES, split_axis=0, concat_axis=0, tiled=True)
        mine = mine.reshape(groups * snps, width // CHUNKS)
        other = lax.ppermute(mine, "core", [(0, 1), (1, 0)])
        product = multiply(left, mine, other, core.reshape(1), rows_n, factor)
        product = product.reshape(rows_n * cores, block_rows // cores, width // CHUNKS)
        product = lax.all_to_all(product, ("x", "zl", "core"), 0, 0, tiled=True)
        news.append(product.reshape(rows_n, cores, block_rows // cores, width // CHUNKS))
    return add(slab_in, news)


def solution(mesh):
    fine = Mesh(mesh.devices.reshape(4, 2, 2, 4, 2), DEVICES)
    row, col = ("x", "zl"), ("zh", "y", "core")
    return jax.shard_map(
        local,
        mesh=fine,
        in_specs=(P(None, row + col, None), P(), P(row, col)),
        out_specs=P(row, col),
        check_vma=False,
    )
```

```python
import functools
import math

import jax
import jax.numpy as jnp
from jax import lax
from jax.experimental import pallas as pl
from jax.experimental.pallas import tpu as pltpu
from jax.sharding import Mesh, PartitionSpec as P


DEVICES = ("x", "zl", "zh", "y", "core")
RINGS = {"x": ("x", (0, 1, 2, 3)), "z": (("zl", "zh"), (0, 2, 1, 3)), "y": ("y", (0, 1, 2, 3))}
ORDERS = (("x", "z", "y"), ("x", "y", "z"), ("z", "y", "x"))
PARTS = ((1, 0, 8), (0, 0, 4), (0, 4, 8))
HALVES = 2
STEP_BLOCKS = 2
SENT = jnp.bfloat16


def neighbour(ring, by):
    axes, order = ring
    here = lax.axis_index(axes)
    found = [order[(order.index(i) + by) % len(order)] for i in range(len(order))]
    return sum(jnp.where(here == i, found[i], 0) for i in range(len(order)))


def turn(block, ring, way):
    axes, order = ring
    axes = axes if isinstance(axes, tuple) else (axes,)
    pairs = []
    for i in range(len(order)):
        pairs.append((2 * order[i], 2 * order[(i + way) % len(order)]))
        pairs.append((2 * order[i] + 1, 2 * order[(i - way) % len(order)] + 1))
    return lax.ppermute(block, axes + ("core",), pairs)


def indices(ring):
    core = lax.axis_index("core")
    before, after = neighbour(ring, -1), neighbour(ring, 1)
    return jnp.stack(
        [
            neighbour(ring, 0),
            jnp.where(core == 0, before, after),
            jnp.where(core == 0, after, before),
            neighbour(ring, 2),
        ]
    )


def chips_order(order):
    weight = {"x": 16, "z": 4, "y": 1}
    first, second, third = (weight[n] * indices(RINGS[n]) for n in order)
    return (third[:, None, None] + second[:, None] + first).reshape(-1)


def gather_rings(blocks, rings):
    ones = [turn(block, RINGS[name], 1) for block, name in zip(blocks, rings, strict=True)]
    others = [turn(block, RINGS[name], -1) for block, name in zip(blocks, rings, strict=True)]
    fars = [turn(block, RINGS[name], 1) for block, name in zip(ones, rings, strict=True)]
    return list(zip(blocks, ones, others, fars, strict=True))


def joined(four, start=None, stop=None):
    return jnp.concatenate([block[:, start:stop] for block in four], axis=0)


def gather_rows(rows, edges):
    second, third = edges[1], edges[2]
    ab, c = gather_rings([rows[:, :third], rows[:, third:]], "xz")
    bc = jnp.concatenate([joined(ab, second), joined(c)], axis=1)
    a, bc = gather_rings([joined(ab, 0, second), bc], "zy")
    held = gather_rings([joined(bc, 0, third - second), joined(bc, third - second)], "zx")
    return gather_rings([joined(a)], "y") + held


def mark_kernel(table, out):
    out[...] = table[...]


def mark(table):
    return pl.pallas_call(
        mark_kernel, out_shape=jax.ShapeDtypeStruct(table.shape, table.dtype), name="mark"
    )(table)


def spread_kernel(dosages, centre, inverse, out):
    groups, own, wide = dosages.shape
    values = dosages[...].astype(jnp.float32).reshape(groups * own, wide)
    values = ((values - centre[...]) * inverse[...]).astype(jnp.bfloat16)
    pieces, places, _, width = out.shape
    for g in range(places):
        for k in range(pieces):
            at = (g * pieces + k) * width
            out[k, g] = values[:, at : at + width]


def spread_columns(dosages, centre, inverse, pieces, places, width):
    groups, own, _ = dosages.shape
    many = 4
    return pl.pallas_call(
        spread_kernel,
        grid=(places // many,),
        in_specs=[
            pl.BlockSpec((groups, own, many * pieces * width), lambda g: (0, 0, g)),
            pl.BlockSpec((groups * own, 1), lambda g: (0, 0)),
            pl.BlockSpec((groups * own, 1), lambda g: (0, 0)),
        ],
        out_specs=pl.BlockSpec((pieces, many, groups * own, width), lambda g: (0, g, 0, 0)),
        out_shape=jax.ShapeDtypeStruct((pieces, places, groups * own, width), jnp.bfloat16),
        cost_estimate=pl.CostEstimate(
            flops=4 * dosages.size, bytes_accessed=4 * dosages.size, transcendentals=0
        ),
        name="spread_columns",
    )(dosages, centre.reshape(-1, 1), inverse.reshape(-1, 1))


def multiply_kernel(scale, starts, parts, cores, slots, chips, *refs):
    lefts, columns, (out, right) = refs[: 4 * len(parts)], refs[4 * len(parts) :], refs[-2:]
    many, variants, _ = columns[0].shape
    step = pl.program_id(0)
    blocks, _, height, _ = out.shape
    for i, part in enumerate(parts):

        @pl.when(step == starts[i])
        def _(part=part):
            def copy(t, carry):
                to = pl.ds(pl.multiple_of(t * variants, variants), variants)
                chip = chips[part, t]
                for c in range(cores):
                    right[c, to, :] = columns[c][chip]
                return carry

            lax.fori_loop(0, many, copy, 0, unroll=8)

        @pl.when(jnp.logical_and(step >= starts[i], step < starts[i + 1]))
        def _(i=i):
            left = jnp.concatenate([ref[...] for ref in lefts[4 * i : 4 * i + 4]], axis=0)
            for c in range(cores):
                product = lax.dot_general(
                    left, right[c], (((0,), (0,)), ((), ())), preferred_element_type=jnp.float32
                )
                product = (scale * product).astype(out.dtype)
                slot = 0 if cores == 1 else slots[c]
                for b in range(blocks):
                    out[b, slot] = product[b * height : (b + 1) * height]


def multiply(held, parts, columns, slots, chips, scale, height, before=None):
    many, variants, width = columns[0].shape
    cores = len(columns)
    wide = STEP_BLOCKS * height
    steps = [four[0].shape[1] // wide for four in held]
    starts = [sum(steps[:i]) for i in range(len(steps) + 1)]
    depth, rows = many * variants, starts[-1] * wide

    def at(i):
        return lambda s, *_: (0, jnp.clip(s - starts[i], 0, steps[i] - 1))

    def to(s, slots, _):
        return (s, slots[0] if cores == 1 else 0, 0, 0)

    given = [] if before is None else [before]
    pieces = [piece for four in held for piece in four]
    return pl.pallas_call(
        functools.partial(multiply_kernel, scale, starts, parts, cores),
        grid_spec=pltpu.PrefetchScalarGridSpec(
            num_scalar_prefetch=2,
            grid=(starts[-1],),
            in_specs=[
                pl.BlockSpec((piece.shape[0], wide), at(i))
                for i, four in enumerate(held)
                for piece in four
            ]
            + [pl.BlockSpec(c.shape, lambda s, *_: (0, 0, 0)) for c in columns]
            + [pl.BlockSpec(memory_space=pl.ANY) for _ in given],
            out_specs=pl.BlockSpec((STEP_BLOCKS, cores, height, width), to),
            scratch_shapes=[pltpu.VMEM((cores, depth, width), columns[0].dtype)],
        ),
        out_shape=jax.ShapeDtypeStruct((rows // height, 2, height, width), SENT),
        input_output_aliases={2 + len(pieces) + cores: 0} if given else {},
        compiler_params=pltpu.CompilerParams(vmem_limit_bytes=(24 + 20 * cores) * 2**20),
        cost_estimate=pl.CostEstimate(
            flops=2 * depth * rows * width * cores,
            bytes_accessed=2 * depth * (rows + width * cores) + 2 * rows * width * cores,
            transcendentals=0,
        ),
        name="multiply",
    )(jnp.stack(slots), chips, *pieces, *columns, *given)


def add_kernel(slab, new, *refs):
    out = refs[-1]
    pieces, _, _, width = new.shape
    for j in range(pieces):
        at = (slice(None), pl.ds(j * width, width))
        out[at] = slab[at] + new[j, 0].astype(jnp.float32)


def add(slab, new, half, before=None):
    pieces, cores, height, width = new.shape
    given = [] if before is None else [before]
    return pl.pallas_call(
        add_kernel,
        grid=(cores,),
        in_specs=[
            pl.BlockSpec((height, slab.shape[1]), lambda c: (c * HALVES + half, 0)),
            pl.BlockSpec((pieces, 1, height, width), lambda c: (0, c, 0, 0)),
        ]
        + [pl.BlockSpec(memory_space=pl.ANY) for _ in given],
        out_specs=pl.BlockSpec((height, slab.shape[1]), lambda c: (c * HALVES + half, 0)),
        out_shape=jax.ShapeDtypeStruct(slab.shape, slab.dtype),
        input_output_aliases={2: 0} if given else {},
        compiler_params=pltpu.CompilerParams(vmem_limit_bytes=60 * 2**20),
        cost_estimate=pl.CostEstimate(
            flops=slab.size, bytes_accessed=5 * slab.size, transcendentals=0
        ),
        name="add_slab",
    )(slab, new, *given)


def local(dosages, allele_counts, slab_in):
    groups, own, samples = dosages.shape
    snps = allele_counts.shape[1]
    rows_n = lax.axis_size("x") * lax.axis_size("zl")
    cores = lax.axis_size("core")
    cols_n = lax.axis_size("zh") * lax.axis_size("y") * cores
    devices = rows_n * cols_n
    block_rows = slab_in.shape[0]
    rows = rows_n * block_rows
    width = samples // devices
    factor = 1.0 / math.sqrt(groups * snps)

    device = lax.axis_index(DEVICES)
    core = lax.axis_index("core")
    counts = lax.dynamic_slice(allele_counts, (0, device * own), (groups, own))
    frequency = counts.astype(jnp.float32) / (2.0 * samples)
    centre = 2.0 * frequency
    inverse = 1.0 / jnp.sqrt(2.0 * frequency * (1.0 - frequency))

    head = dosages[:, :, :rows].astype(jnp.float32)
    head = ((head - centre[:, :, None]) * inverse[:, :, None]).astype(jnp.bfloat16)
    height = block_rows // cores // HALVES
    head = head.reshape(groups * own, rows_n, cores, HALVES, height).transpose(2, 0, 3, 1, 4)
    head = jnp.concatenate(
        [head[:, :, h, b0:b1].reshape(cores, groups * own, -1) for h, b0, b1 in PARTS], axis=2
    )
    head = lax.all_to_all(head, "core", split_axis=0, concat_axis=0, tiled=True)
    head = head.reshape(cores * groups * own, rows // cores)
    sizes = [height * (b1 - b0) for _, b0, b1 in PARTS]
    held = gather_rows(head, [sum(sizes[:i]) for i in range(len(sizes) + 1)])

    columns = spread_columns(dosages, centre, inverse, rows_n, cols_n, width)
    columns = columns.reshape(devices, groups * own, width)
    mine = lax.all_to_all(columns, DEVICES, split_axis=0, concat_axis=0, tiled=True)
    mine = mine.reshape(devices // cores, cores * groups * own, width)
    other = lax.ppermute(mine, "core", [(0, 1), (1, 0)])

    chips = jnp.stack([chips_order(order) for order in ORDERS]).astype(jnp.int32)
    chips = mark(chips)
    out = None
    for half in range(HALVES):
        parts = [i for i, part in enumerate(PARTS) if part[0] == half]
        pieces = [held[i] for i in parts]
        if half == 0:
            product = multiply(pieces, parts, [mine], [core], chips, factor, height)
            product = multiply(pieces, parts, [other], [1 - core], chips, factor, height, product)
        else:
            product = multiply(
                pieces, parts, [mine, other], [core, 1 - core], chips, factor, height
            )
        product = product.reshape(rows_n * cores, height, width)
        product = lax.all_to_all(product, ("x", "zl", "core"), 0, 0, tiled=True)
        product = product.reshape(rows_n, cores, height, width)
        out = add(slab_in, product, half, out)
    return out


def solution(mesh):
    fine = Mesh(mesh.devices.reshape(4, 2, 2, 4, 2), DEVICES)
    row, col = ("x", "zl"), ("zh", "y", "core")

    return jax.shard_map(
        local,
        mesh=fine,
        in_specs=(P(None, row + col, None), P(), P(row, col)),
        out_specs=P(row, col),
        check_vma=False,
    )
```
